32 devices in a mesh: row: 8 (over z, x), col: 4 (over y, core).
Axes of the slice: x: 2, y: 2, z: 4, core: 2. Of those that a mesh axis runs over, the one named last changes fastest.
Arguments:
- hidden: bfloat16 [4, 20480, 768], P(None, ('row', 'col')), may hold values from -6 to 6
- grad_out: bfloat16 [4, 20480, 1024], P(None, ('row', 'col')), may hold values from -6 to 6
- counts: int32 [32, 4], P(('row', 'col')), may hold values from 1 to 640, as said below
- shadow_ids: int32 [4], replicated, may hold values from 0 to 59, as said below
- master: float32 [60, 768, 1024], P(None, 'row', 'col'), may hold values from -0.21875 to 0.21875
- momentum: float32 [60, 768, 1024], P(None, 'row', 'col'), may hold values from -6 to 6
Outputs:
- master_out: float32 [60, 768, 1024], P(None, 'row', 'col')
- momentum_out: float32 [60, 768, 1024], P(None, 'row', 'col')
- shadow_out: bfloat16 [4, 768, 1024], P(None, 'row')
The draws below stay inside these ranges and needn't reach their ends.
Inputs may be any that keep to these rules, and one draw needn't show every extreme that they name: counts are at most 640, and some device reaches 640 for some shadowed expert. `shadow_ids`: the 4 ids are distinct, and experts 0 and 59 are always among them.
All inputs are finite; a program needn't handle non-finite values.
Results may differ from the reference program's by a relative error of at most 0.007.
Values may be sent and summed in bfloat16 or wider, within the bound.
A program may use at most 128 MiB of HBM per device.

```python
import jax
import jax.numpy as jnp
from jax import lax

D_WIN = 1024
F_WIN = 768
EXPERTS = 60
SHADOW = 4
CAP = 640
TOKENS = 20480
N_ROW = 8
N_COL = 4


def draw_counts(key, part):
    devices = N_ROW * N_COL
    first = jax.random.randint(jax.random.fold_in(key, 11), (devices, SHADOW), 1, CAP + 1)
    second = jax.random.randint(jax.random.fold_in(key, 12), (devices, SHADOW), 1, CAP + 1)
    values = jnp.minimum(first, second)
    chosen = jax.random.randint(jax.random.fold_in(key, 13), (), 0, devices * SHADOW)
    flat_index = jnp.arange(devices * SHADOW, dtype=jnp.int32).reshape(devices, SHADOW)
    return jnp.where(flat_index == chosen, CAP, values).astype(jnp.int32)


def draw_shadow_ids(key, part):
    middle = jax.random.permutation(jax.random.fold_in(key, 21), EXPERTS - 2) + 1
    ends = jnp.array([0, EXPERTS - 1], dtype=jnp.int32)
    chosen = jnp.concatenate([ends, middle[:SHADOW - 2].astype(jnp.int32)])
    return jax.random.permutation(jax.random.fold_in(key, 22), chosen).astype(jnp.int32)


def raised(values, rng, source, target, shards_of, factor):
    owner, partner = [(jnp.arange(values.shape[dim]) // (values.shape[dim] // shards_of)).reshape([-1 if axis == dim else 1 for axis in range(values.ndim)]) for dim in (source, target)]
    chosen = jax.random.permutation(rng, shards_of)[partner]
    strong = (owner == chosen) | (owner == (partner + shards_of // 2) % shards_of)
    return jnp.where(strong, factor * values, values)


def levels(rng, dims, pieces, smallest, high):
    level, own = 1.0, jax.random.fold_in(rng, 6)
    for axis_at, blocks in pieces:
        draws = jnp.exp(jax.random.uniform(jax.random.fold_in(own, axis_at), (blocks,), jnp.float32, smallest / len(pieces), high / len(pieces)))
        level = level * jnp.repeat(draws, dims[axis_at] // blocks).reshape([-1 if axis == axis_at else 1 for axis in range(len(dims))])
    return level


def gaussian(key, dims, spread, limit, cuts=(), kind=jnp.bfloat16):
    gain = levels(key, dims, cuts, -0.22, 0.18) if cuts else 1.0
    drawn = jax.random.normal(key, dims, jnp.float32) * spread * gain
    return jnp.minimum(jnp.maximum(drawn, -limit), limit).astype(kind)


def gaussian_with(stream_key, dims, width, most, cuts, heavy, kind=jnp.bfloat16):
    values = width * jax.random.normal(stream_key, dims, jnp.float32)
    if cuts:
        values = values * levels(stream_key, dims, cuts, -0.22, 0.18)
    return jnp.clip(raised(values, jax.random.fold_in(stream_key, 3), *heavy), -most, most).astype(kind)


def setup_inputs(seed: int = 0) -> dict:
    key_list = jax.random.split(jax.random.key(seed), 7)
    hidden = gaussian(key_list[0], (SHADOW, TOKENS, F_WIN), 1.0, 6.0, ((1, 32),))
    grad_out = gaussian_with(key_list[1], (SHADOW, TOKENS, D_WIN), 1.0, 6.0, ((1, 32),), (1, 2, 32, 2.75))
    counts = draw_counts(jax.random.fold_in(key_list[6], 71), 0)
    shadow_ids = draw_shadow_ids(jax.random.fold_in(key_list[6], 71), 0)
    master = gaussian(key_list[4], (EXPERTS, F_WIN, D_WIN), F_WIN ** -0.5, 0.21875, ((1, 8), (2, 4)), jnp.float32)
    momentum = gaussian(key_list[5], (EXPERTS, F_WIN, D_WIN), 1.0, 6.0, ((1, 8), (2, 4)), jnp.float32)
    return dict(hidden=hidden, grad_out=grad_out, counts=counts, shadow_ids=shadow_ids, master=master, momentum=momentum)


def reference(hidden, grad_out, counts, shadow_ids, master, momentum):
    devices = N_ROW * N_COL
    positions = jnp.arange(CAP, dtype=jnp.int32)

    def one_expert(expert):
        live_mask = (positions[None, :] < counts[:, expert][:, None]).reshape(-1)
        masked = jnp.where(live_mask[:, None], hidden[expert], jnp.zeros((), jnp.bfloat16))
        return jnp.dot(masked.T, grad_out[expert], preferred_element_type=jnp.float32)

    gradient = lax.map(one_expert, jnp.arange(SHADOW, dtype=jnp.int32))
    gradient = gradient * jnp.float32((CAP * devices) ** -0.5)
    new_momentum = 0.9 * momentum[shadow_ids] + gradient
    new_master = master[shadow_ids] - 0.01 * new_momentum
    momentum_out = momentum.at[shadow_ids].set(new_momentum)
    master_out = master.at[shadow_ids].set(new_master)
    return master_out, momentum_out, new_master.astype(jnp.bfloat16)
```

```python
import functools

import jax
import jax.numpy as jnp
from jax import lax
from jax.experimental import pallas as pl
from jax.experimental.pallas import tpu as pltpu
from jax.sharding import PartitionSpec as P

momentum_decay = 0.9
step_size = 0.01
bf16, f32 = jnp.bfloat16, jnp.float32
MESH = pl.DeviceIdType.MESH


def gather_body(ids, w_ref, m_ref, w_out, m_out):
    w_out[...] = w_ref[...]
    m_out[...] = m_ref[...]


def scatter_body(ids, w_new, m_new, w_any, m_any, w_out, m_out):
    w_out[...] = w_new[...]
    m_out[...] = m_new[...]


def reduce_body(sizes, counts, hidden, grad, w_rows, m_rows, w_new, m_new, shadow,
                h_in, g_in, h_t, part, r_core, s_core, rx1, sx1, rx2, ry1, sy1, ry2, s_last, r_last,
                in_sem, core_sem, one_sem, two_sem, last_sem, ag_sem, fw_sem):
    experts, cap, outer_row, outer_col, feat, width, halves, scale = sizes
    chunks = experts * halves
    row, col = lax.axis_index("row"), lax.axis_index("col")
    z, x = row // 2, row % 2
    y, core = col // 2, col % 2

    def spots(name):
        if name == "core":
            return [(1 - core, (row, y * 2 + 1 - core))]
        if name == "x":
            return [(1 - x, (z * 2 + 1 - x, col))]
        if name == "y":
            others = [lax.rem(y + d, outer_col) for d in range(1, outer_col)]
            return [(t, (row, t * 2 + core)) for t in others]
        others = [lax.rem(z + d, outer_row) for d in range(1, outer_row)]
        return [(t, (t * 2 + x, col)) for t in others]

    loads = []
    for e in range(experts):
        pair = (
            pltpu.make_async_copy(hidden.at[e], h_in.at[e], in_sem.at[0, e]),
            pltpu.make_async_copy(grad.at[e], g_in.at[e], in_sem.at[1, e]),
        )
        for copy in pair:
            copy.start()
        loads.append(pair)

    barrier = pltpu.get_barrier_semaphore()
    greeted = [where for name in ("core", "x", "y", "z") for _, where in spots(name)]
    for where in greeted:
        pl.semaphore_signal(barrier, inc=1, device_id=where, device_id_type=MESH)

    started = []

    def send(src, dst, sem, where):
        copy = pltpu.make_async_remote_copy(
            src_ref=src, dst_ref=dst, send_sem=sem.at[0], recv_sem=sem.at[1],
            device_id=where, device_id_type=MESH,
        )
        copy.start()
        started.append(copy)
        return copy

    flight = {}

    def multiply(e):
        for copy in loads[e]:
            copy.wait()
        live = lax.broadcasted_iota(jnp.int32, (cap, h_in.shape[2]), 0) < counts[0, e]
        h_t[...] = jnp.where(live, h_in[e], jnp.zeros((), bf16)).T
        block = halves * width
        step = max(256, block)
        for first in range(0, g_in.shape[2], step):
            got = jnp.dot(h_t[...], g_in[e, :, first:first + step], preferred_element_type=f32).astype(bf16)
            for k in range(step // block):
                at = first // block + k
                for h in range(halves):
                    cut = got[:, k * block + h * width:k * block + (h + 1) * width]
                    part[e * halves + h, at // 2, at % 2] = cut.reshape(outer_row, 2, feat, width)
        if e == 0:
            pl.semaphore_wait(barrier, len(greeted))
        for h in range(halves):
            c = e * halves + h
            ((t, where),) = spots("core")
            flight["core", c] = [send(part.at[c, :, t], r_core.at[c], core_sem.at[c], where)]

    def first(c):
        for copy in flight["core", c]:
            copy.wait_recv()
        for b in range(outer_col):
            s_core[c, b] = (part[c, b, core].astype(f32) + r_core[c, b].astype(f32)).astype(bf16)
        i = c // 2
        if c % 2 == 0:
            ((t, where),) = spots("x")
            flight["one", c] = [send(s_core.at[c, :, :, t], rx1.at[i], one_sem.at[c, 0], where)]
        else:
            flight["one", c] = [
                send(s_core.at[c, t], ry1.at[i, d], one_sem.at[c, d], where)
                for d, (t, where) in enumerate(spots("y"))
            ]

    def second(c):
        for copy in flight["one", c]:
            copy.wait_recv()
        i = c // 2
        if c % 2 == 0:
            for b in range(outer_col):
                sx1[i, b] = (s_core[c, b, :, x].astype(f32) + rx1[i, b].astype(f32)).astype(bf16)
            flight["two", c] = [
                send(sx1.at[i, t], rx2.at[i, d], two_sem.at[c, d], where)
                for d, (t, where) in enumerate(spots("y"))
            ]
        else:
            total = s_core[c, y].astype(f32)
            for d in range(outer_col - 1):
                total = total + ry1[i, d].astype(f32)
            sy1[i] = total.astype(bf16)
            ((t, where),) = spots("x")
            flight["two", c] = [send(sy1.at[i, :, t], ry2.at[i], two_sem.at[c, 0], where)]

    def third(c):
        for copy in flight["two", c]:
            copy.wait_recv()
        i = c // 2
        if c % 2 == 0:
            total = sx1[i, y].astype(f32)
            for d in range(outer_col - 1):
                total = total + rx2[i, d].astype(f32)
        else:
            total = sy1[i, :, x].astype(f32) + ry2[i].astype(f32)
        s_last[c] = total.astype(bf16)
        flight["last", c] = [
            send(s_last.at[c, t], r_last.at[c, d], last_sem.at[c, d], where)
            for d, (t, where) in enumerate(spots("z"))
        ]

    def fourth(c):
        for copy in flight["last", c]:
            copy.wait_recv()
        total = s_last[c, z].astype(f32)
        for d in range(outer_row - 1):
            total = total + r_last[c, d].astype(f32)
        e, lanes = c // halves, slice(c % halves * width, (c % halves + 1) * width)
        moved = momentum_decay * m_rows[e, :, lanes] + total * f32(scale)
        m_new[e, :, lanes] = moved
        stepped = w_rows[e, :, lanes] - step_size * moved
        w_new[e, :, lanes] = stepped
        shadow[y, core, c] = stepped.astype(bf16)
        own = shadow.at[y, core, c]
        flight["ag", c] = [
            send(own, own, ag_sem.at[c, d], where) for d, (t, where) in enumerate(spots("y"))
        ]

    def fifth(c):
        for copy in flight["ag", c]:
            copy.wait_recv()
        ((t, where),) = spots("core")
        ours = shadow.at[:, core, c]
        flight["fw", c] = [send(ours, ours, fw_sem.at[c], where)]

    stages = (first, second, third, fourth, fifth)
    plan = [("m", 0), ("m", 1), (0, 0), ("m", 2), (0, 1)]
    plan += [("m", e) for e in range(3, experts)]
    for tick in range(experts + 4):
        for stage, e in ((1, tick), (2, tick - 1), (0, tick + 2), (3, tick - 2), (4, tick - 3)):
            if 0 <= e < experts:
                plan.append((stage, e))
    for stage, e in plan:
        if stage == "m":
            multiply(e)
            continue
        for h in range(halves):
            stages[stage](e * halves + h)
    for c in range(chunks):
        for copy in flight["fw", c]:
            copy.wait_recv()
    for copy in started:
        copy.wait_send()


def shards(hidden, grad_out, counts, shadow_ids, master, momentum):
    experts, cap, hid = hidden.shape
    out = grad_out.shape[2]
    n_row, n_col = lax.axis_size("row"), lax.axis_size("col")
    feat, block = master.shape[1:]
    halves = 2 if block % 256 == 0 else 1
    width = block // halves
    chunks = experts * halves
    outer_row, outer_col = n_row // 2, n_col // 2
    scale = (cap * n_row * n_col) ** (-0.5)
    pairs = (chunks + 1) // 2

    row_of = pl.BlockSpec((1, feat, block), lambda i, ids: (ids[i], 0, 0))
    row_at = pl.BlockSpec((1, feat, block), lambda i, ids: (i, 0, 0))
    rows_type = jax.ShapeDtypeStruct((experts, feat, block), f32)
    w_rows, m_rows = pl.pallas_call(
        gather_body,
        grid_spec=pltpu.PrefetchScalarGridSpec(
            num_scalar_prefetch=1, grid=(experts,), in_specs=[row_of, row_of], out_specs=[row_at, row_at]
        ),
        out_shape=[rows_type, rows_type],
        name="pick_rows",
    )(shadow_ids, master, momentum)

    sizes = (experts, cap, outer_row, outer_col, feat, width, halves, scale)
    tail = (feat, width)
    oc1, or1 = max(outer_col - 1, 1), max(outer_row - 1, 1)
    vmem = pl.BlockSpec(memory_space=pltpu.VMEM)
    anywhere = pl.BlockSpec(memory_space=pl.ANY)
    dma = pltpu.SemaphoreType.DMA
    w_new, m_new, shadow = pl.pallas_call(
        functools.partial(reduce_body, sizes),
        in_specs=[pl.BlockSpec(memory_space=pltpu.SMEM), anywhere, anywhere, vmem, vmem],
        out_specs=[vmem, vmem, vmem],
        out_shape=[rows_type, rows_type, jax.ShapeDtypeStruct((outer_col, 2, chunks) + tail, bf16)],
        scratch_shapes=[
            pltpu.VMEM((experts, cap, hid), bf16),
            pltpu.VMEM((experts, cap, out), bf16),
            pltpu.VMEM((hid, cap), bf16),
            pltpu.VMEM((chunks, outer_col, 2, outer_row, 2) + tail, bf16),
            pltpu.VMEM((chunks, outer_col, outer_row, 2) + tail, bf16),
            pltpu.VMEM((chunks, outer_col, outer_row, 2) + tail, bf16),
            pltpu.VMEM((pairs, outer_col, outer_row) + tail, bf16),
            pltpu.VMEM((pairs, outer_col, outer_row) + tail, bf16),
            pltpu.VMEM((pairs, oc1, outer_row) + tail, bf16),
            pltpu.VMEM((pairs, oc1, outer_row, 2) + tail, bf16),
            pltpu.VMEM((pairs, outer_row, 2) + tail, bf16),
            pltpu.VMEM((pairs, outer_row) + tail, bf16),
            pltpu.VMEM((chunks, outer_row) + tail, bf16),
            pltpu.VMEM((chunks, or1) + tail, bf16),
            dma((2, experts)),
            dma((chunks, 2)),
            dma((chunks, oc1, 2)),
            dma((chunks, oc1, 2)),
            dma((chunks, or1, 2)),
            dma((chunks, oc1, 2)),
            dma((chunks, 2)),
        ],
        compiler_params=pltpu.CompilerParams(
            collective_id=0, has_side_effects=True, vmem_limit_bytes=60 * 1024 * 1024
        ),
        cost_estimate=pl.CostEstimate(
            flops=2 * experts * cap * hid * out, bytes_accessed=2 * experts * cap * (hid + out), transcendentals=0
        ),
        name="reduce_step",
    )(counts, hidden, grad_out, w_rows, m_rows)

    master_out, momentum_out = pl.pallas_call(
        scatter_body,
        grid_spec=pltpu.PrefetchScalarGridSpec(
            num_scalar_prefetch=1, grid=(experts,),
            in_specs=[row_at, row_at, anywhere, anywhere], out_specs=[row_of, row_of],
        ),
        out_shape=[jax.ShapeDtypeStruct(master.shape, f32)] * 2,
        input_output_aliases={3: 0, 4: 1},
        name="put_rows",
    )(shadow_ids, w_new, m_new, master, momentum)
    shadow = shadow.reshape(n_col, experts, halves, feat, width)
    shadow_out = shadow.transpose(1, 3, 0, 2, 4).reshape(experts, feat, out)
    return (master_out, momentum_out, shadow_out)


def solution(mesh):
    return jax.shard_map(
        shards,
        mesh=mesh,
        in_specs=(
            P(None, ("row", "col"), None),
            P(None, ("row", "col"), None),
            P(("row", "col"), None),
            P(),
            P(None, "row", "col"),
            P(None, "row", "col"),
        ),
        out_specs=(P(None, "row", "col"), P(None, "row", "col"), P(None, "row", None)),
        check_vma=False,
    )
```

```python
import functools

import jax
import jax.numpy as jnp
from jax import lax
from jax.experimental import pallas as pl
from jax.experimental.pallas import tpu as pltpu
from jax.sharding import PartitionSpec as P

momentum_decay = 0.9
step_size = 0.01
bf16, f32 = jnp.bfloat16, jnp.float32
MESH = pl.DeviceIdType.MESH


def table_body(ids, w_new, m_new, w_in, m_in, w_out, m_out, w_stage, m_stage, sem):
    reads = [
        pltpu.make_async_copy(w_in, w_stage, sem.at[0]),
        pltpu.make_async_copy(m_in, m_stage, sem.at[1]),
    ]
    writes = [
        pltpu.make_async_copy(w_stage, w_out, sem.at[2]),
        pltpu.make_async_copy(m_stage, m_out, sem.at[3]),
    ]
    for copy in reads:
        copy.start()
    for read, stage, rows, write in zip(reads, (w_stage, m_stage), (w_new, m_new), writes):
        read.wait()
        for e in range(rows.shape[0]):
            stage[ids[e]] = rows[e]
        write.start()
    for copy in writes:
        copy.wait()


def reduce_body(sizes, counts, ids, hidden, grad, master, momentum, w_new, m_new, shadow_out,
                shadow, w_stage, m_stage, h_in, g_in, h_t, part, r_core, s_core, rx1, sx1, rx2, ry1, sy1, ry2, s_last, r_last,
                in_sem, table_sem, core_sem, one_sem, two_sem, last_sem, ag_sem, fw_sem):
    experts, cap, outer_row, outer_col, feat, width, halves, scale = sizes
    chunks = experts * halves
    row, col = lax.axis_index("row"), lax.axis_index("col")
    z, x = row // 2, row % 2
    y, core = col // 2, col % 2

    def spots(name):
        if name == "core":
            return [(1 - core, (row, y * 2 + 1 - core))]
        if name == "x":
            return [(1 - x, (z * 2 + 1 - x, col))]
        if name == "y":
            others = [lax.rem(y + d, outer_col) for d in range(1, outer_col)]
            return [(t, (row, t * 2 + core)) for t in others]
        others = [lax.rem(z + d, outer_row) for d in range(1, outer_row)]
        return [(t, (t * 2 + x, col)) for t in others]

    loads = []
    for e in range(experts):
        pair = (
            pltpu.make_async_copy(hidden.at[e], h_in.at[e], in_sem.at[0, e]),
            pltpu.make_async_copy(grad.at[e], g_in.at[e], in_sem.at[1, e]),
        )
        for copy in pair:
            copy.start()
        loads.append(pair)
    reads = [
        pltpu.make_async_copy(master, w_stage, table_sem.at[0]),
        pltpu.make_async_copy(momentum, m_stage, table_sem.at[1]),
    ]
    for copy in reads:
        copy.start()

    barrier = pltpu.get_barrier_semaphore()
    greeted = [where for name in ("core", "x", "y", "z") for _, where in spots(name)]
    for where in greeted:
        pl.semaphore_signal(barrier, inc=1, device_id=where, device_id_type=MESH)

    started = []

    def send(src, dst, sem, where):
        copy = pltpu.make_async_remote_copy(
            src_ref=src, dst_ref=dst, send_sem=sem.at[0], recv_sem=sem.at[1],
            device_id=where, device_id_type=MESH,
        )
        copy.start()
        started.append(copy)
        return copy

    flight = {}

    def multiply(e):
        for copy in loads[e]:
            copy.wait()
        live = lax.broadcasted_iota(jnp.int32, (cap, h_in.shape[2]), 0) < counts[0, e]
        h_t[...] = jnp.where(live, h_in[e], jnp.zeros((), bf16)).T
        block = halves * width
        step = max(256, block)
        for first in range(0, g_in.shape[2], step):
            got = jnp.dot(h_t[...], g_in[e, :, first:first + step], preferred_element_type=f32).astype(bf16)
            for k in range(step // block):
                at = first // block + k
                for h in range(halves):
                    cut = got[:, k * block + h * width:k * block + (h + 1) * width]
                    part[e * halves + h, at // 2, at % 2] = cut.reshape(outer_row, 2, feat, width)
        if e == 0:
            pl.semaphore_wait(barrier, len(greeted))
        for h in range(halves):
            c = e * halves + h
            ((t, where),) = spots("core")
            flight["core", c] = [send(part.at[c, :, t], r_core.at[c], core_sem.at[c], where)]

    def first(c):
        for copy in flight["core", c]:
            copy.wait_recv()
        for b in range(outer_col):
            s_core[c, b] = (part[c, b, core].astype(f32) + r_core[c, b].astype(f32)).astype(bf16)
        i = c // 2
        if c % 2 == 0:
            ((t, where),) = spots("x")
            flight["one", c] = [send(s_core.at[c, :, :, t], rx1.at[i], one_sem.at[c, 0], where)]
        else:
            flight["one", c] = [
                send(s_core.at[c, t], ry1.at[i, d], one_sem.at[c, d], where)
                for d, (t, where) in enumerate(spots("y"))
            ]

    def second(c):
        for copy in flight["one", c]:
            copy.wait_recv()
        i = c // 2
        if c % 2 == 0:
            for b in range(outer_col):
                sx1[i, b] = (s_core[c, b, :, x].astype(f32) + rx1[i, b].astype(f32)).astype(bf16)
            flight["two", c] = [
                send(sx1.at[i, t], rx2.at[i, d], two_sem.at[c, d], where)
                for d, (t, where) in enumerate(spots("y"))
            ]
        else:
            total = s_core[c, y].astype(f32)
            for d in range(outer_col - 1):
                total = total + ry1[i, d].astype(f32)
            sy1[i] = total.astype(bf16)
            ((t, where),) = spots("x")
            flight["two", c] = [send(sy1.at[i, :, t], ry2.at[i], two_sem.at[c, 0], where)]

    def third(c):
        for copy in flight["two", c]:
            copy.wait_recv()
        i = c // 2
        if c % 2 == 0:
            total = sx1[i, y].astype(f32)
            for d in range(outer_col - 1):
                total = total + rx2[i, d].astype(f32)
        else:
            total = sy1[i, :, x].astype(f32) + ry2[i].astype(f32)
        s_last[c] = total.astype(bf16)
        flight["last", c] = [
            send(s_last.at[c, t], r_last.at[c, d], last_sem.at[c, d], where)
            for d, (t, where) in enumerate(spots("z"))
        ]

    def fourth(c):
        for copy in flight["last", c]:
            copy.wait_recv()
        total = s_last[c, z].astype(f32)
        for d in range(outer_row - 1):
            total = total + r_last[c, d].astype(f32)
        e, lanes = c // halves, slice(c % halves * width, (c % halves + 1) * width)
        moved = momentum_decay * m_stage[ids[e], :, lanes] + total * f32(scale)
        m_new[e, :, lanes] = moved
        stepped = w_stage[ids[e], :, lanes] - step_size * moved
        w_new[e, :, lanes] = stepped
        shadow[y, core, c] = stepped.astype(bf16)
        own = shadow.at[y, core, c]
        flight["ag", c] = [
            send(own, own, ag_sem.at[c, d], where) for d, (t, where) in enumerate(spots("y"))
        ]

    def fifth(c):
        for copy in flight["ag", c]:
            copy.wait_recv()
        ((t, where),) = spots("core")
        ours = shadow.at[:, core, c]
        flight["fw", c] = [send(ours, ours, fw_sem.at[c], where)]

    stages = (first, second, third, fourth, fifth)
    plan = [("m", 0), ("m", 1), (0, 0), ("m", 2), (0, 1)]
    plan += [("m", e) for e in range(3, experts)]
    for tick in range(experts + 4):
        for stage, e in ((1, tick), (2, tick - 1), (0, tick + 2), (3, tick - 2), (4, tick - 3)):
            if 0 <= e < experts:
                plan.append((stage, e))
    for stage, e in plan:
        if stage == "m":
            multiply(e)
            if e == experts - 1:
                for read in reads:
                    read.wait()
            continue
        for h in range(halves):
            stages[stage](e * halves + h)
    for c in range(chunks):
        for copy in flight["fw", c]:
            copy.wait_recv()
        e, h = c // halves, c % halves
        for b in range(outer_col):
            for t in range(2):
                at = ((b * 2 + t) * halves + h) * width
                shadow_out[e, :, at:at + width] = shadow[b, t, c]
    for copy in started:
        copy.wait_send()


def shards(hidden, grad_out, counts, shadow_ids, master, momentum):
    experts, cap, hid = hidden.shape
    out = grad_out.shape[2]
    n_row, n_col = lax.axis_size("row"), lax.axis_size("col")
    feat, block = master.shape[1:]
    halves = 2 if block % 256 == 0 else 1
    width = block // halves
    chunks = experts * halves
    outer_row, outer_col = n_row // 2, n_col // 2
    scale = (cap * n_row * n_col) ** (-0.5)
    pairs = (chunks + 1) // 2

    rows_type = jax.ShapeDtypeStruct((experts, feat, block), f32)
    table_type = jax.ShapeDtypeStruct(master.shape, f32)
    sizes = (experts, cap, outer_row, outer_col, feat, width, halves, scale)
    tail = (feat, width)
    oc1, or1 = max(outer_col - 1, 1), max(outer_row - 1, 1)
    vmem = pl.BlockSpec(memory_space=pltpu.VMEM)
    anywhere = pl.BlockSpec(memory_space=pl.ANY)
    dma = pltpu.SemaphoreType.DMA
    w_new, m_new, shadow_out = pl.pallas_call(
        functools.partial(reduce_body, sizes),
        in_specs=[pl.BlockSpec(memory_space=pltpu.SMEM)] * 2 + [anywhere] * 4,
        out_specs=[vmem] * 3,
        out_shape=[rows_type] * 2 + [jax.ShapeDtypeStruct((experts, feat, out), bf16)],
        scratch_shapes=[
            pltpu.VMEM((outer_col, 2, chunks) + tail, bf16),
            pltpu.VMEM(master.shape, f32),
            pltpu.VMEM(master.shape, f32),
            pltpu.VMEM((experts, cap, hid), bf16),
            pltpu.VMEM((experts, cap, out), bf16),
            pltpu.VMEM((hid, cap), bf16),
            pltpu.VMEM((chunks, outer_col, 2, outer_row, 2) + tail, bf16),
            pltpu.VMEM((chunks, outer_col, outer_row, 2) + tail, bf16),
            pltpu.VMEM((chunks, outer_col, outer_row, 2) + tail, bf16),
            pltpu.VMEM((pairs, outer_col, outer_row) + tail, bf16),
            pltpu.VMEM((pairs, outer_col, outer_row) + tail, bf16),
            pltpu.VMEM((pairs, oc1, outer_row) + tail, bf16),
            pltpu.VMEM((pairs, oc1, outer_row, 2) + tail, bf16),
            pltpu.VMEM((pairs, outer_row, 2) + tail, bf16),
            pltpu.VMEM((pairs, outer_row) + tail, bf16),
            pltpu.VMEM((chunks, outer_row) + tail, bf16),
            pltpu.VMEM((chunks, or1) + tail, bf16),
            dma((2, experts)),
            dma((2,)),
            dma((chunks, 2)),
            dma((chunks, oc1, 2)),
            dma((chunks, oc1, 2)),
            dma((chunks, or1, 2)),
            dma((chunks, oc1, 2)),
            dma((chunks, 2)),
        ],
        compiler_params=pltpu.CompilerParams(
            collective_id=0, has_side_effects=True, vmem_limit_bytes=60 * 1024 * 1024
        ),
        cost_estimate=pl.CostEstimate(
            flops=2 * experts * cap * hid * out, bytes_accessed=2 * experts * cap * (hid + out), transcendentals=0
        ),
        name="reduce_step",
    )(counts, shadow_ids, hidden, grad_out, master, momentum)

    master_out, momentum_out = pl.pallas_call(
        table_body,
        in_specs=[pl.BlockSpec(memory_space=pltpu.SMEM), vmem, vmem, anywhere, anywhere],
        out_specs=[anywhere, anywhere],
        out_shape=[table_type] * 2,
        scratch_shapes=[pltpu.VMEM(master.shape, f32), pltpu.VMEM(master.shape, f32), dma((4,))],
        name="put_rows",
    )(shadow_ids, w_new, m_new, master, momentum)
    return (master_out, momentum_out, shadow_out)


def solution(mesh):
    return jax.shard_map(
        shards,
        mesh=mesh,
        in_specs=(
            P(None, ("row", "col"), None),
            P(None, ("row", "col"), None),
            P(("row", "col"), None),
            P(),
            P(None, "row", "col"),
            P(None, "row", "col"),
        ),
        out_specs=(P(None, "row", "col"), P(None, "row", "col"), P(None, "row", None)),
        check_vma=False,
    )
```
